1024 devices in a mesh: ep: 16 (over z, core), dp: 64 (over x, y).
Axes of the slice: x: 8, y: 8, z: 8, core: 2. Of those that a mesh axis runs over, the one named last changes fastest.
Arguments:
- tokens: bfloat16 [2048, 7168], P('dp', 'ep'), may hold values from -6 to 6
- gate_weight: bfloat16 [64, 7168, 1024], P('dp', 'ep'), may hold values from -0.0625 to 0.0625
- up_weight: bfloat16 [64, 7168, 1024], P('dp', 'ep'), may hold values from -0.0625 to 0.0625
- down_weight: bfloat16 [64, 1024, 7168], P('dp', None, 'ep'), may hold values from -0.1875 to 0.1875
- targets: int32 [2048, 8], P('dp'), may hold values from 0 to 63, all different within a row; in each aligned block of 32 rows (0 to 31, 32 to 63, ...) at most 8 rows name the same one
- mixing: float32 [2048, 8], P('dp'), may hold values from 0.05 to 1
- move_plan: int32 [64], replicated, may hold values from 0 to 63, as said below
Outputs:
- mixed: bfloat16 [2048, 7168], P('dp', 'ep')
The draws below stay inside these ranges and needn't reach their ends.
Inputs may be any that keep to these rules, and one draw needn't show every extreme that they name: `targets`: each row names 8 different slots; within the 32 rows of one token group no slot is named more than 8 times, and in some groups one slot exactly 8 times. `move_plan`: every entry is either its own slot or one common source slot; the source serves its own copy; the slot after the source and the slot half of 64 after it (cyclically) always serve the source's copy, and each other slot does so with probability one half.
All inputs are finite; a program needn't handle non-finite values.
Results may differ from the reference program's by a relative error of at most 0.0058.
Values may be sent and summed in bfloat16 or wider, within the bound.
No kernel may reach another device: no remote copies, remote signals or barrier semaphores. Data moves between devices by JAX's collectives and lax.ppermute only.
A program may use at most 32 MiB of HBM per device.

```python
import math
import jax
import jax.numpy as jnp
import numpy as np
from jax import lax

D = 7168
FF = 1024
TOP = 8
TOK_G = 32
CAP = 8
TOKENS = 2048
N_EP = 16
N_DP = 64


def draw_move_plan(key, part):
    first, second = jax.random.split(jax.random.fold_in(key, 7))
    source_slot = jax.random.randint(first, (), 0, N_DP)
    slots_all = jnp.arange(N_DP, dtype=jnp.int32)
    offset = (slots_all - source_slot) % N_DP
    coins = jax.random.randint(second, (N_DP,), 0, 2)
    served = (offset != 0) & ((coins == 1) | (offset == 1) | (offset == N_DP // 2))
    return jnp.where(served, source_slot, slots_all).astype(jnp.int32)


def steps_of(rng, extent, cuts, smallest, largest):
    factor_of = 1.0
    for position, blocks in cuts:
        draws = jax.random.uniform(jax.random.fold_in(jax.random.fold_in(rng, 6), position), (blocks,), jnp.float32, smallest / len(cuts), largest / len(cuts))
        factor_of = factor_of * jnp.repeat(jnp.exp(draws), extent[position] // blocks).reshape((-1,) + (1,) * (len(extent) - 1 - position))
    return factor_of


def assign_block(stream_key, own, number, rows, count, top, bound, slope):
    ranking = jax.random.permutation(stream_key, count)
    crowded, ordinary = load_shares(count, rows * top, bound, slope, True), load_shares(count, rows * top, bound, slope, False)
    places = jnp.arange(count)

    def named(lengths, turn):
        used = int((lengths > 0).sum())
        fixed = max(1, used // 4)
        passed = fixed + (places - fixed + turn * (used - fixed)) % max(1, count - fixed)
        return jnp.zeros((count,), jnp.int32).at[ranking[jnp.where(places < fixed, places, passed)]].set(jnp.asarray(lengths, jnp.int32))

    lengths = jnp.where(number % 4 == 0, named(crowded, number // 4), named(ordinary, number - number // 4 - 1))
    mixed = jax.random.permutation(jax.random.fold_in(own, 3), count)
    giver, receiver = mixed[0:count // 2 * 2:2], mixed[1:count // 2 * 2:2]
    slack = jnp.minimum(lengths[giver] - 1, bound - lengths[receiver]) // 2
    slack = jnp.where((giver == ranking[0]) | (receiver == ranking[0]) | (lengths[receiver] == 0), 0, jnp.maximum(slack, 0))
    passed = jax.random.randint(jax.random.fold_in(own, 4), (count // 2,), 0, 1 << 20) % (slack + 1)
    lengths = lengths.at[giver].add(-passed).at[receiver].add(passed)
    labels = jnp.searchsorted(jnp.cumsum(lengths), jnp.arange(rows * top), side="right").astype(jnp.int32)
    listing = labels.reshape(top, rows).T
    listing = listing[jax.random.permutation(jax.random.fold_in(own, 1), rows)]
    turn = jax.random.randint(jax.random.fold_in(own, 2), (rows, 1), 0, top)
    return jnp.take_along_axis(listing, (jnp.arange(top)[None, :] + turn) % top, axis=1)


def load_shares(amount, total, reach, slope, full):
    portions = [(1 << 20) // math.isqrt(rank ** slope) + 1 for rank in range(1, amount + 1)]
    largest = reach if full else min(reach, max(-(-total // amount), total * portions[0] // sum(portions)))
    least = 1 if total - largest >= amount - 1 else 0
    given, surplus = [largest] + [least] * (amount - 1), total - largest - least * (amount - 1)
    while surplus > 0:
        free = [i for i in range(1, amount) if given[i] < largest] or [i for i in range(1, amount) if given[i] < reach]
        whole, remaining = sum([portions[i] for i in free]), surplus
        for i in free:
            addition = min(reach - given[i], max(1, remaining * portions[i] // whole), surplus)
            given[i] = given[i] + addition
            surplus = surplus - addition
    return np.array(given)


def bell_draw(rng, shape, deviation, reach, shards=(), held_as=jnp.bfloat16):
    array = jax.random.normal(rng, shape, jnp.float32) * deviation
    if len(shards) > 0:
        array = steps_of(rng, shape, shards, -0.22, 0.18) * array
    return jnp.clip(array, min=-reach, max=reach).astype(held_as)


def setup_inputs(seed: int = 0) -> dict:
    streams_of = jax.random.split(jax.random.key(seed), 8)
    tokens = bell_draw(streams_of[0], (TOKENS, D), 1.0, 6.0, ((0, 64), (1, 16)))
    gate_weight = bell_draw(streams_of[1], (N_DP, D, FF), D ** -0.5, 0.0625, ((0, 64), (1, 16)))
    up_weight = bell_draw(streams_of[2], (N_DP, D, FF), D ** -0.5, 0.0625, ((0, 64), (1, 16)))
    down_weight = bell_draw(streams_of[3], (N_DP, FF, D), FF ** -0.5, 0.1875, ((0, 64), (2, 16)))
    targets_keys = jax.random.split(jax.random.fold_in(streams_of[4], 1), TOKENS // TOK_G)
    targets_turns = jax.random.permutation(jax.random.fold_in(streams_of[4], 3), TOKENS // TOK_G)
    targets = jax.vmap(lambda own, number: assign_block(jax.random.fold_in(streams_of[4], 2), own, number, TOK_G, N_DP, TOP, CAP, 2))(targets_keys, targets_turns).reshape((TOKENS, TOP))
    mixing = jnp.clip(jnp.exp(math.log(1.0) - 2.9957323 * jax.random.uniform(streams_of[5], (TOKENS, TOP), jnp.float32) ** steps_of(streams_of[5], (TOKENS, TOP), ((0, 64),), -0.2, 0.2)), 0.05, 1.0)
    move_plan = draw_move_plan(jax.random.fold_in(streams_of[7], 71), 0)
    return dict(tokens=tokens, gate_weight=gate_weight, up_weight=up_weight, down_weight=down_weight, targets=targets, mixing=mixing, move_plan=move_plan)


def run_expert(rows, gate_cols, up_cols, down_rows):
    count = rows.shape[0]
    width = D // N_EP
    blocks = rows.reshape(count, N_EP, width).astype(jnp.float32)
    gate_blocks = gate_cols.reshape(N_EP, width, FF).astype(jnp.float32)
    up_blocks = up_cols.reshape(N_EP, width, FF).astype(jnp.float32)
    gate = jnp.einsum("nbd,bdf->nf", blocks, gate_blocks)
    up = jnp.einsum("nbd,bdf->nf", blocks, up_blocks)
    hidden = (jax.nn.silu(gate) * up).astype(jnp.bfloat16)
    return jnp.dot(hidden, down_rows, preferred_element_type=jnp.float32).astype(jnp.bfloat16)


def reference(tokens, gate_weight, up_weight, down_weight, targets, mixing, move_plan):
    flat_targets = targets.reshape(-1).astype(jnp.int32)
    flat_mixing = mixing.reshape(-1)
    slots = N_DP * CAP
    places = jnp.arange(slots, dtype=jnp.int32)
    plan = move_plan.astype(jnp.int32)

    def visit(total, group):
        anchor = plan[group].astype(jnp.int32)
        gate_cols = lax.dynamic_index_in_dim(gate_weight, anchor, 0, keepdims=False)
        up_cols = lax.dynamic_index_in_dim(up_weight, anchor, 0, keepdims=False)
        down_rows = lax.dynamic_index_in_dim(down_weight, anchor, 0, keepdims=False)
        chosen = flat_targets == group
        found = jnp.nonzero(chosen, size=slots, fill_value=0)[0].astype(jnp.int32)
        live = places < jnp.sum(chosen.astype(jnp.int32))
        owners = (found // TOP).astype(jnp.int32)
        result = run_expert(tokens[owners], gate_cols, up_cols, down_rows).astype(jnp.float32)
        scale = jnp.where(live, flat_mixing[found], 0.0)
        return total.at[owners].add(result * scale[:, None]), None

    start = jnp.zeros((TOKENS, D), jnp.float32)
    total, unused = lax.scan(visit, start, jnp.arange(N_DP, dtype=jnp.int32))
    return total.astype(jnp.bfloat16)
```

```python
import jax
import jax.numpy as jnp
from jax import lax
from jax.sharding import Mesh
from jax.sharding import PartitionSpec as P

CHIPS_Z, CORES, CHIPS_X, CHIPS_Y = 8, 2, 8, 8


def scatter_from(pieces, axis, count, source):
    me = lax.axis_index(axis)

    def branch(root):
        def run(blocks):
            total = jnp.where(me == root, blocks[root], jnp.zeros_like(blocks[root]))
            for other in range(count):
                if other != root:
                    total = total + lax.ppermute(blocks[other], axis, [(root, other)])
            return total

        return run

    return lax.switch(source, [branch(root) for root in range(count)], pieces)


def copy_from(block, axis, count, source):
    me = lax.axis_index(axis)

    def branch(root):
        def run(mine):
            total = jnp.where(me == root, mine, jnp.zeros_like(mine))
            for other in range(count):
                if other != root:
                    total = total + lax.ppermute(mine, axis, [(root, other)])
            return total

        return run

    return lax.switch(source, [branch(root) for root in range(count)], block)


def dot(left, right):
    return jnp.dot(left, right, preferred_element_type=jnp.float32)


def per_device(tokens, gate_weight, up_weight, down_weight, targets, mixing, move_plan):
    nz, nc, nx, ny = (lax.axis_size(a) for a in ("z", "c", "x", "y"))
    groups, parts = nx * ny, nz * nc
    core, x_index = lax.axis_index("c"), lax.axis_index("x")
    token_rows, per_token = targets.shape
    width = tokens.shape[1]
    hidden_units = gate_weight.shape[2]
    slot_cap = min(token_rows, max(2, (2 * token_rows * per_token + groups - 1) // groups))
    slots = groups * slot_cap
    half, share = slots // nc, slots // parts
    block_units = hidden_units // nx
    lanes = jnp.arange(groups, dtype=jnp.int32)
    source = jnp.max(jnp.where(move_plan != lanes, move_plan, -1))
    gate, up, down = gate_weight[0], up_weight[0], down_weight[0]

    named = (targets[:, :, None] == lanes).astype(jnp.float32)
    moved = ((move_plan == source) | (lanes == source)).astype(jnp.float32)
    from_source = jnp.sum(named * moved, axis=2)
    hits = jnp.sum(named * (1.0 - moved), axis=1)
    rank = jnp.arange(token_rows, dtype=jnp.int32)
    before = (rank[None, :] < rank[:, None]).astype(jnp.bfloat16)
    earlier = dot(before, hits.astype(jnp.bfloat16))
    position = jnp.sum(named * earlier[:, None, :], axis=2).astype(jnp.int32)
    destination = jnp.where(from_source > 0, -1, targets * slot_cap + position)
    places = jnp.arange(slots, dtype=jnp.int32)
    matches = (destination[:, :, None] == places).astype(jnp.float32)
    pick = jnp.sum(matches, axis=1).astype(jnp.bfloat16)
    blend = jnp.sum(matches * mixing[:, :, None], axis=1)
    source_mix = jnp.sum(mixing * from_source, axis=1)

    outgoing = lax.dot_general(
        pick, tokens, (((0,), (0,)), ((), ())), preferred_element_type=jnp.float32
    ).astype(jnp.bfloat16)
    arrived = lax.all_to_all(
        outgoing.reshape(groups, slot_cap, width), ("x", "y"), 0, 0, tiled=True
    ).reshape(slots, width)

    tall = jnp.concatenate([gate, up, down.T], axis=0)
    pieces = jnp.stack(
        [tall[:, i * block_units : (i + 1) * block_units] for i in range(nx)]
    )
    piece = scatter_from(pieces, "x", nx, source // ny)
    line_tokens = lax.all_gather(tokens, "x", axis=0, tiled=True)
    arrived, piece, line_tokens = lax.optimization_barrier((arrived, piece, line_tokens))

    def project(first):
        rows = lax.dynamic_slice_in_dim(arrived, first, half, 0)
        return jnp.concatenate([dot(rows, gate), dot(rows, up)], axis=1)

    swap = [(0, 1), (1, 0)]
    sent = lax.ppermute(project((1 - core) * half).astype(jnp.bfloat16), "c", swap)
    chip_sum = (project(core * half) + sent.astype(jnp.float32)).astype(jnp.bfloat16)
    chip_sum, piece = lax.optimization_barrier((chip_sum, piece))
    spread = lax.all_to_all(
        chip_sum.reshape(nz, share, 2 * hidden_units), "z", 0, 0, tiled=True
    )
    piece = copy_from(piece, "y", ny, source % ny)
    spread, piece = lax.optimization_barrier((spread, piece))
    summed = jnp.sum(spread.astype(jnp.float32), axis=0)
    hidden = (jax.nn.silu(summed[:, :hidden_units]) * summed[:, hidden_units:]).astype(jnp.bfloat16)

    gate_block, up_block, down_block = piece[:width], piece[width : 2 * width], piece[2 * width :]
    line_sums = jnp.concatenate(
        [dot(line_tokens, gate_block), dot(line_tokens, up_block)], axis=1
    ).astype(jnp.bfloat16)
    line_rows = nx * token_rows
    line_share = line_rows // parts
    line_parts = lax.all_to_all(
        line_sums.reshape(parts, line_share, 2 * block_units), ("z", "c"), 0, 0, tiled=True
    )
    line_total = jnp.sum(line_parts.astype(jnp.float32), axis=0)
    line_hidden = (
        jax.nn.silu(line_total[:, :block_units]) * line_total[:, block_units:]
    ).astype(jnp.bfloat16)

    extra = line_share * block_units // hidden_units
    filler = -(share + extra) % 8
    payload = jnp.concatenate(
        [hidden, line_hidden.reshape(extra, hidden_units), jnp.zeros((filler, hidden_units), jnp.bfloat16)]
    )
    mine = lax.all_to_all(
        jnp.broadcast_to(payload, (nz,) + payload.shape), "z", 0, 0, tiled=True
    )
    other = lax.ppermute(mine, "c", swap)

    def outputs(both):
        rows = both[:, :share].reshape(half, hidden_units)
        line = both[:, share : share + extra].reshape(nz * line_share, block_units)
        line_out = lax.dot_general(
            line, down_block, (((1,), (1,)), ((), ())), preferred_element_type=jnp.float32
        )
        return dot(rows, down).astype(jnp.bfloat16), line_out.astype(jnp.bfloat16)

    def in_order(a, b, axis):
        first, second = jnp.where(core == 0, a, b), jnp.where(core == 0, b, a)
        return jnp.concatenate([first, second], axis=axis)

    out_mine, line_mine = outputs(mine)
    out_other, line_other = outputs(other)
    results = in_order(out_mine, out_other, 0)
    returned = lax.all_to_all(
        results.reshape(groups, slot_cap, width), ("x", "y"), 0, 0, tiled=True
    ).reshape(slots, width)
    line_out = in_order(
        line_mine.reshape(nz, line_share, width), line_other.reshape(nz, line_share, width), 1
    )
    line_back = lax.all_to_all(
        line_out.reshape(nx, token_rows, width), "x", 0, 0, tiled=True
    )
    source_out = jnp.sum(line_back.astype(jnp.float32), axis=0).astype(jnp.bfloat16)
    mixed = jnp.dot(blend, returned.astype(jnp.float32), precision=lax.Precision.HIGHEST)
    mixed = mixed + source_mix[:, None] * source_out.astype(jnp.float32)
    return mixed.astype(jnp.bfloat16)


def solution(mesh):
    split = Mesh(
        mesh.devices.reshape(CHIPS_Z, CORES, CHIPS_X, CHIPS_Y), ("z", "c", "x", "y")
    )
    ep, dp = ("z", "c"), ("x", "y")
    return jax.shard_map(
        per_device,
        mesh=split,
        in_specs=(
            P(dp, ep),
            P(dp, ep, None),
            P(dp, ep, None),
            P(dp, None, ep),
            P(dp, None),
            P(dp, None),
            P(),
        ),
        out_specs=P(dp, ep),
        check_vma=False,
    )
```

```python
import jax
import jax.numpy as jnp
from jax import lax
from jax.sharding import Mesh
from jax.sharding import PartitionSpec as P

CHIPS_Z, CORES, CHIPS_X, CHIPS_Y = 8, 2, 8, 8


def from_source(blocks, axis, count, source):
    distance = (lax.axis_index(axis) - source + count) % count

    def branch(parity):
        def run(sent):
            kept = sent[0]
            for k in range(1, count):
                pairs = [(root, (root + k) % count) for root in range(parity, count, 2)]
                kept = jnp.where(distance == k, lax.ppermute(sent[k], axis, pairs), kept)
            return kept

        return run

    return lax.switch(source % 2, [branch(0), branch(1)], blocks)


def sum_over_line(blocks, axis, count):
    me = lax.axis_index(axis)
    bit = 1
    while bit < count:
        mine = (me // bit) % 2
        pairs = [(i, i ^ bit) for i in range(count)]
        split = blocks.reshape((blocks.shape[0] // 2, 2) + blocks.shape[1:])
        kept = lax.dynamic_index_in_dim(split, mine, 1, keepdims=False)
        sent = lax.dynamic_index_in_dim(split, 1 - mine, 1, keepdims=False)
        got = lax.ppermute(sent.astype(jnp.bfloat16), axis, pairs)
        blocks = kept.astype(jnp.float32) + got.astype(jnp.float32)
        bit *= 2
    return blocks[0]


def dot(left, right):
    return jnp.dot(left, right, preferred_element_type=jnp.float32)


def per_device(tokens, gate_weight, up_weight, down_weight, targets, mixing, move_plan):
    nz, nc, nx, ny = (lax.axis_size(a) for a in ("z", "c", "x", "y"))
    groups, parts = nx * ny, nz * nc
    core, x_index = lax.axis_index("c"), lax.axis_index("x")
    token_rows, per_token = targets.shape
    width = tokens.shape[1]
    hidden_units = gate_weight.shape[2]
    slot_cap = min(token_rows, max(2, (2 * token_rows * per_token + groups - 1) // groups))
    slots = groups * slot_cap
    half, share = slots // nc, slots // parts
    block_units = hidden_units // nx
    lanes = jnp.arange(groups, dtype=jnp.int32)
    source = jnp.max(jnp.where(move_plan != lanes, move_plan, -1))
    gate, up, down = gate_weight[0], up_weight[0], down_weight[0]

    named = (targets[:, :, None] == lanes).astype(jnp.float32)
    moved = ((move_plan == source) | (lanes == source)).astype(jnp.float32)
    served = jnp.sum(named * moved, axis=2)
    hits = jnp.sum(named * (1.0 - moved), axis=1)
    rank = jnp.arange(token_rows, dtype=jnp.int32)
    before = (rank[None, :] < rank[:, None]).astype(jnp.bfloat16)
    earlier = dot(before, hits.astype(jnp.bfloat16))
    position = jnp.sum(named * earlier[:, None, :], axis=2).astype(jnp.int32)
    destination = jnp.where(served > 0, -1, targets * slot_cap + position)
    places = jnp.arange(slots, dtype=jnp.int32)
    matches = (destination[:, :, None] == places).astype(jnp.float32)
    pick = jnp.sum(matches, axis=1).astype(jnp.bfloat16)
    blend = jnp.sum(matches * mixing[:, :, None], axis=1)
    source_mix = jnp.sum(mixing * served, axis=1)

    outgoing = lax.dot_general(
        pick, tokens, (((0,), (0,)), ((), ())), preferred_element_type=jnp.float32
    ).astype(jnp.bfloat16)
    line_tokens = lax.all_to_all(
        jnp.broadcast_to(tokens, (nx,) + tokens.shape), "x", 0, 0, tiled=True
    ).reshape(nx * token_rows, width)
    outgoing, line_tokens = lax.optimization_barrier((outgoing, line_tokens))
    arrived = lax.all_to_all(
        outgoing.reshape(groups, slot_cap, width), ("x", "y"), 0, 0, tiled=True
    ).reshape(slots, width)

    tall = jnp.concatenate([gate, up, down.T], axis=0)
    pieces = jnp.stack(
        [tall[:, i * block_units : (i + 1) * block_units] for i in range(nx)]
    )
    turned = [
        lax.dynamic_index_in_dim(pieces, (x_index + k) % nx, 0, keepdims=False)
        for k in range(nx)
    ]
    piece = from_source(turned, "x", nx, source // ny)
    arrived, piece = lax.optimization_barrier((arrived, piece))

    def project(first):
        rows = lax.dynamic_slice_in_dim(arrived, first, half, 0)
        return jnp.concatenate([dot(rows, gate), dot(rows, up)], axis=1)

    swap = [(0, 1), (1, 0)]
    sent = lax.ppermute(project((1 - core) * half).astype(jnp.bfloat16), "c", swap)
    chip_sum = (project(core * half) + sent.astype(jnp.float32)).astype(jnp.bfloat16)
    chip_sum, piece = lax.optimization_barrier((chip_sum, piece))
    spread = lax.all_to_all(
        chip_sum.reshape(nz, share, 2 * hidden_units), "z", 0, 0, tiled=True
    )
    piece = from_source([piece] * ny, "y", ny, source % ny)
    spread, piece = lax.optimization_barrier((spread, piece))
    summed = jnp.sum(spread.astype(jnp.float32), axis=0)
    hidden = (jax.nn.silu(summed[:, :hidden_units]) * summed[:, hidden_units:]).astype(jnp.bfloat16)

    gate_block, up_block, down_block = piece[:width], piece[width : 2 * width], piece[2 * width :]
    line_sums = jnp.concatenate(
        [dot(line_tokens, gate_block), dot(line_tokens, up_block)], axis=1
    ).astype(jnp.bfloat16)
    line_rows = nx * token_rows
    line_share = line_rows // parts
    line_parts = lax.all_to_all(
        line_sums.reshape(parts, line_share, 2 * block_units), ("z", "c"), 0, 0, tiled=True
    )
    line_total = jnp.sum(line_parts.astype(jnp.float32), axis=0)
    line_hidden = (
        jax.nn.silu(line_total[:, :block_units]) * line_total[:, block_units:]
    ).astype(jnp.bfloat16)

    extra = line_share * block_units // hidden_units
    filler = -(share + extra) % 8
    payload = jnp.concatenate(
        [hidden, line_hidden.reshape(extra, hidden_units), jnp.zeros((filler, hidden_units), jnp.bfloat16)]
    )
    mine = lax.all_to_all(
        jnp.broadcast_to(payload, (nz,) + payload.shape), "z", 0, 0, tiled=True
    )
    other = lax.ppermute(mine, "c", swap)

    def outputs(both):
        rows = both[:, :share].reshape(half, hidden_units)
        line = both[:, share : share + extra].reshape(nz * line_share, block_units)
        line_out = lax.dot_general(
            line, down_block, (((1,), (1,)), ((), ())), preferred_element_type=jnp.float32
        )
        return dot(rows, down).astype(jnp.bfloat16), line_out

    def in_order(a, b, axis):
        first, second = jnp.where(core == 0, a, b), jnp.where(core == 0, b, a)
        return jnp.concatenate([first, second], axis=axis)

    out_mine, line_mine = outputs(mine)
    out_other, line_other = outputs(other)
    results = in_order(out_mine, out_other, 0)
    line_out = in_order(
        line_mine.reshape(nz, line_share, width), line_other.reshape(nz, line_share, width), 1
    )
    results, line_out = lax.optimization_barrier((results, line_out))
    returned = lax.all_to_all(
        results.reshape(groups, slot_cap, width), ("x", "y"), 0, 0, tiled=True
    ).reshape(slots, width)
    source_out = sum_over_line(line_out.reshape(nx, token_rows, width), "x", nx)
    source_out = source_out.astype(jnp.bfloat16)
    mixed = jnp.dot(blend, returned.astype(jnp.float32), precision=lax.Precision.HIGHEST)
    mixed = mixed + source_mix[:, None] * source_out.astype(jnp.float32)
    return mixed.astype(jnp.bfloat16)


def solution(mesh):
    split = Mesh(
        mesh.devices.reshape(CHIPS_Z, CORES, CHIPS_X, CHIPS_Y), ("z", "c", "x", "y")
    )
    ep, dp = ("z", "c"), ("x", "y")
    return jax.shard_map(
        per_device,
        mesh=split,
        in_specs=(
            P(dp, ep),
            P(dp, ep, None),
            P(dp, ep, None),
            P(dp, None, ep),
            P(dp, None),
            P(dp, None),
            P(),
        ),
        out_specs=P(dp, ep),
        check_vma=False,
    )
```

```python
import jax
import jax.numpy as jnp
from jax import lax
from jax.sharding import Mesh
from jax.sharding import PartitionSpec as P

CHIPS_Z, CORES, CHIPS_X, CHIPS_Y = 8, 2, 8, 8


def from_source(blocks, axis, count, source):
    distance = (lax.axis_index(axis) - source + count) % count
    classes = min(4, count)

    def branch(first):
        def run(sent):
            kept = sent[0]
            for k in range(1, count):
                pairs = [(root, (root + k) % count) for root in range(first, count, classes)]
                kept = jnp.where(distance == k, lax.ppermute(sent[k], axis, pairs), kept)
            return kept

        return run

    return lax.switch(source % classes, [branch(i) for i in range(classes)], blocks)


def spread_from(block, axis, count, source):
    parts = block.reshape((count, block.shape[0] // count) + block.shape[1:])
    part = lax.dynamic_index_in_dim(
        lax.all_to_all(parts, axis, 0, 0, tiled=True), source, 0, keepdims=False
    )
    whole = lax.all_to_all(
        jnp.broadcast_to(part, (count,) + part.shape), axis, 0, 0, tiled=True
    )
    return whole.reshape(block.shape)


def dot(left, right):
    return jnp.dot(left, right, preferred_element_type=jnp.float32)


def per_device(tokens, gate_weight, up_weight, down_weight, targets, mixing, move_plan):
    nz, nc, nx, ny = (lax.axis_size(a) for a in ("z", "c", "x", "y"))
    groups, parts = nx * ny, nz * nc
    core = lax.axis_index("c")
    token_rows, per_token = targets.shape
    width = tokens.shape[1]
    hidden_units = gate_weight.shape[2]
    slot_cap = min(token_rows, max(2, (2 * token_rows * per_token + groups - 1) // groups))
    slots = groups * slot_cap
    half, share = slots // nc, slots // parts
    block_units = hidden_units // nx
    lanes = jnp.arange(groups, dtype=jnp.int32)
    source = jnp.max(jnp.where(move_plan != lanes, move_plan, -1))
    gate, up, down = gate_weight[0], up_weight[0], down_weight[0]

    named = (targets[:, :, None] == lanes).astype(jnp.float32)
    moved = ((move_plan == source) | (lanes == source)).astype(jnp.float32)
    served = jnp.sum(named * moved, axis=2)
    hits = jnp.sum(named * (1.0 - moved), axis=1)
    rank = jnp.arange(token_rows, dtype=jnp.int32)
    before = (rank[None, :] < rank[:, None]).astype(jnp.bfloat16)
    earlier = dot(before, hits.astype(jnp.bfloat16))
    position = jnp.sum(named * earlier[:, None, :], axis=2).astype(jnp.int32)
    destination = jnp.where(served > 0, -1, targets * slot_cap + position)
    places = jnp.arange(slots, dtype=jnp.int32)
    matches = (destination[:, :, None] == places).astype(jnp.float32)
    pick = jnp.sum(matches, axis=1).astype(jnp.bfloat16)
    blend = jnp.sum(matches * mixing[:, :, None], axis=1)
    source_mix = jnp.sum(mixing * served, axis=1)

    outgoing = lax.dot_general(
        pick, tokens, (((0,), (0,)), ((), ())), preferred_element_type=jnp.float32
    ).astype(jnp.bfloat16)
    line_tokens = lax.all_to_all(
        jnp.broadcast_to(tokens, (nx,) + tokens.shape), "x", 0, 0, tiled=True
    ).reshape(nx * token_rows, width)
    outgoing, line_tokens = lax.optimization_barrier((outgoing, line_tokens))
    arrived = lax.all_to_all(
        outgoing.reshape(groups, slot_cap, width), ("x", "y"), 0, 0, tiled=True
    ).reshape(slots, width)

    tall = jnp.concatenate([gate, up, down.T], axis=0)
    pieces = [tall[:, k * block_units : (k + 1) * block_units] for k in range(nx)]
    piece = from_source(pieces, "x", nx, source // ny)
    arrived, piece = lax.optimization_barrier((arrived, piece))
    piece = spread_from(piece, "y", ny, source % ny)
    gate_block, up_block, down_block = piece[:width], piece[width : 2 * width], piece[2 * width :]

    swap = [(0, 1), (1, 0)]
    line_share = nx * token_rows // parts
    line_rows = line_tokens.reshape(nz, nc, line_share, width)

    def project(side):
        rows = lax.dynamic_slice_in_dim(arrived, side * half, half, 0)
        sums = jnp.concatenate([dot(rows, gate), dot(rows, up)], axis=1)
        return sums.reshape(nz, share, 2 * hidden_units)

    def project_line(side):
        rows = lax.dynamic_index_in_dim(line_rows, side, 1, keepdims=False)
        rows = rows.reshape(nz * line_share, width)
        sums = [dot(rows, w).reshape(nz, line_share, block_units) for w in (gate_block, up_block)]
        return jnp.concatenate(sums, axis=1)

    def chip_sums(function):
        other = lax.ppermute(function(1 - core).astype(jnp.bfloat16), "c", swap)
        return (function(core) + other.astype(jnp.float32)).astype(jnp.bfloat16)

    def lanes_for(value, count):
        missing = count - value.shape[-2]
        edges = [(0, 0)] * (value.ndim - 2) + [(0, missing), (0, 0)]
        return jnp.pad(value, edges) if missing else value

    tall_rows = max(share, 2 * line_share)
    joined = jnp.concatenate(
        [lanes_for(chip_sums(project), tall_rows), lanes_for(chip_sums(project_line), tall_rows)],
        axis=2,
    )
    spread = lax.all_to_all(joined, "z", 0, 0, tiled=True)
    summed = jnp.sum(spread.astype(jnp.float32), axis=0)
    main, line = summed[:share, : 2 * hidden_units], summed[: 2 * line_share, 2 * hidden_units :]
    hidden = (jax.nn.silu(main[:, :hidden_units]) * main[:, hidden_units:]).astype(jnp.bfloat16)
    line_hidden = (jax.nn.silu(line[:line_share]) * line[line_share:]).astype(jnp.bfloat16)

    rows_sent = max(share, line_share)
    payload = jnp.concatenate(
        [lanes_for(hidden, rows_sent), lanes_for(line_hidden, rows_sent)], axis=1
    )
    mine = lax.all_to_all(
        jnp.broadcast_to(payload, (nz,) + payload.shape), "z", 0, 0, tiled=True
    )
    other = lax.ppermute(mine, "c", swap)

    def line_outputs(both):
        rows = both[:, :line_share, hidden_units:].reshape(nz * line_share, block_units)
        out = lax.dot_general(
            rows, down_block, (((1,), (1,)), ((), ())), preferred_element_type=jnp.float32
        )
        return out.astype(jnp.bfloat16).reshape(nz, line_share, width)

    def outputs(both):
        rows = both[:, :share, :hidden_units].reshape(half, hidden_units)
        return dot(rows, down).astype(jnp.bfloat16)

    def in_order(a, b, axis):
        first, second = jnp.where(core == 0, a, b), jnp.where(core == 0, b, a)
        return jnp.concatenate([first, second], axis=axis)

    line_out = in_order(line_outputs(mine), line_outputs(other), 1)
    line_back = lax.all_to_all(
        line_out.reshape(nx, token_rows, width), "x", 0, 0, tiled=True
    )
    results = in_order(outputs(mine), outputs(other), 0)
    returned = lax.all_to_all(
        results.reshape(groups, slot_cap, width), ("x", "y"), 0, 0, tiled=True
    ).reshape(slots, width)
    source_out = jnp.sum(line_back.astype(jnp.float32), axis=0).astype(jnp.bfloat16)
    mixed = jnp.dot(blend, returned.astype(jnp.float32), precision=lax.Precision.HIGHEST)
    mixed = mixed + source_mix[:, None] * source_out.astype(jnp.float32)
    return mixed.astype(jnp.bfloat16)


def solution(mesh):
    split = Mesh(
        mesh.devices.reshape(CHIPS_Z, CORES, CHIPS_X, CHIPS_Y), ("z", "c", "x", "y")
    )
    ep, dp = ("z", "c"), ("x", "y")
    return jax.shard_map(
        per_device,
        mesh=split,
        in_specs=(
            P(dp, ep),
            P(dp, ep, None),
            P(dp, ep, None),
            P(dp, None, ep),
            P(dp, None),
            P(dp, None),
            P(),
        ),
        out_specs=P(dp, ep),
        check_vma=False,
    )
```

```python
import jax
import jax.numpy as jnp
from jax import lax
from jax.sharding import Mesh
from jax.sharding import PartitionSpec as P

CHIPS_Z, CORES, CHIPS_X, CHIPS_Y = 8, 2, 8, 8


def from_source(blocks, axis, count, source):
    distance = (lax.axis_index(axis) - source + count) % count
    classes = min(4, count)

    def branch(first):
        def run(sent):
            kept = sent[0]
            for k in range(1, count):
                apart = 2 if k in (1, count - 1) else classes
                pairs = [(root, (root + k) % count) for root in range(first % apart, count, apart)]
                kept = jnp.where(distance == k, lax.ppermute(sent[k], axis, pairs), kept)
            return kept

        return run

    return lax.switch(source % classes, [branch(i) for i in range(classes)], blocks)


def relay_from(block, axis, count, source, chains=2):
    distance = (lax.axis_index(axis) - source + count) % count
    ahead = [(i, (i + 1) % count) for i in range(count)]
    back = [(i, (i - 1) % count) for i in range(count)]
    held = jnp.split(block, chains)
    for step in range(1, count // 2 + 1):
        for part in range(chains):
            sent = held[part]
            kept = jnp.where(distance == step, lax.ppermute(sent, axis, ahead), sent)
            if step < count - step:
                got = lax.ppermute(sent, axis, back)
                kept = jnp.where(distance == count - step, got, kept)
            held[part] = kept
    return jnp.concatenate(held)


def dot(left, right):
    return jnp.dot(left, right, preferred_element_type=jnp.float32)


def per_device(tokens, gate_weight, up_weight, down_weight, targets, mixing, move_plan):
    nz, nc, nx, ny = (lax.axis_size(a) for a in ("z", "c", "x", "y"))
    groups, parts = nx * ny, nz * nc
    core = lax.axis_index("c")
    token_rows, per_token = targets.shape
    width = tokens.shape[1]
    hidden_units = gate_weight.shape[2]
    slot_cap = min(token_rows, max(2, (2 * token_rows * per_token + groups - 1) // groups))
    slots = groups * slot_cap
    half, share = slots // nc, slots // parts
    block_units = hidden_units // nx
    lanes = jnp.arange(groups, dtype=jnp.int32)
    source = jnp.max(jnp.where(move_plan != lanes, move_plan, -1))
    gate, up, down = gate_weight[0], up_weight[0], down_weight[0]

    named = (targets[:, :, None] == lanes).astype(jnp.float32)
    moved = ((move_plan == source) | (lanes == source)).astype(jnp.float32)
    served = jnp.sum(named * moved, axis=2)
    hits = jnp.sum(named * (1.0 - moved), axis=1)
    rank = jnp.arange(token_rows, dtype=jnp.int32)
    before = (rank[None, :] < rank[:, None]).astype(jnp.bfloat16)
    earlier = dot(before, hits.astype(jnp.bfloat16))
    position = jnp.sum(named * earlier[:, None, :], axis=2).astype(jnp.int32)
    destination = jnp.where(served > 0, -1, targets * slot_cap + position)
    places = jnp.arange(slots, dtype=jnp.int32)
    matches = (destination[:, :, None] == places).astype(jnp.float32)
    pick = jnp.sum(matches, axis=1).astype(jnp.bfloat16)
    blend = jnp.sum(matches * mixing[:, :, None], axis=1)
    source_mix = jnp.sum(mixing * served, axis=1)

    outgoing = lax.dot_general(
        pick, tokens, (((0,), (0,)), ((), ())), preferred_element_type=jnp.float32
    ).astype(jnp.bfloat16)
    line_tokens = lax.all_to_all(
        jnp.broadcast_to(tokens, (nx,) + tokens.shape), "x", 0, 0, tiled=True
    ).reshape(nx * token_rows, width)
    outgoing, line_tokens = lax.optimization_barrier((outgoing, line_tokens))
    arrived = lax.all_to_all(
        outgoing.reshape(groups, slot_cap, width), ("x", "y"), 0, 0, tiled=True
    ).reshape(slots, width)

    tall = jnp.concatenate([gate, up, down.T], axis=0)
    pieces = [tall[:, k * block_units : (k + 1) * block_units] for k in range(nx)]
    piece = from_source(pieces, "x", nx, source // ny)
    arrived, piece = lax.optimization_barrier((arrived, piece))

    swap = [(0, 1), (1, 0)]

    def project(side):
        rows = lax.dynamic_slice_in_dim(arrived, side * half, half, 0)
        return jnp.concatenate([dot(rows, gate), dot(rows, up)], axis=1)

    sent = lax.ppermute(project(1 - core).astype(jnp.bfloat16), "c", swap)
    chip_sum = (project(core) + sent.astype(jnp.float32)).astype(jnp.bfloat16)
    spread = lax.all_to_all(
        chip_sum.reshape(nz, share, 2 * hidden_units), "z", 0, 0, tiled=True
    )
    piece = relay_from(piece, "y", ny, source % ny)
    spread, piece = lax.optimization_barrier((spread, piece))
    gate_block, up_block, down_block = piece[:width], piece[width : 2 * width], piece[2 * width :]

    line_share = nx * token_rows // parts
    line_sums = jnp.concatenate(
        [dot(line_tokens, gate_block), dot(line_tokens, up_block)], axis=1
    ).astype(jnp.bfloat16)
    line_parts = lax.all_to_all(
        line_sums.reshape(parts, line_share, 2 * block_units), ("z", "c"), 0, 0, tiled=True
    )
    main = jnp.sum(spread.astype(jnp.float32), axis=0)
    hidden = (jax.nn.silu(main[:, :hidden_units]) * main[:, hidden_units:]).astype(jnp.bfloat16)
    line = jnp.sum(line_parts.astype(jnp.float32), axis=0)
    line_hidden = (jax.nn.silu(line[:, :block_units]) * line[:, block_units:]).astype(jnp.bfloat16)

    def lanes_for(value, count):
        missing = count - value.shape[0]
        return jnp.pad(value, ((0, missing), (0, 0))) if missing else value

    rows_sent = max(share, line_share)
    payload = jnp.concatenate(
        [lanes_for(hidden, rows_sent), lanes_for(line_hidden, rows_sent)], axis=1
    )
    mine = lax.all_to_all(
        jnp.broadcast_to(payload, (nz,) + payload.shape), "z", 0, 0, tiled=True
    )
    other = lax.ppermute(mine, "c", swap)

    def line_outputs(both):
        rows = both[:, :line_share, hidden_units:].reshape(nz * line_share, block_units)
        out = lax.dot_general(
            rows, down_block, (((1,), (1,)), ((), ())), preferred_element_type=jnp.float32
        )
        return out.astype(jnp.bfloat16).reshape(nz, line_share, width)

    def outputs(both):
        rows = both[:, :share, :hidden_units].reshape(half, hidden_units)
        return dot(rows, down).astype(jnp.bfloat16)

    def in_order(a, b, axis):
        first, second = jnp.where(core == 0, a, b), jnp.where(core == 0, b, a)
        return jnp.concatenate([first, second], axis=axis)

    line_out = in_order(line_outputs(mine), line_outputs(other), 1)
    line_back = lax.all_to_all(
        line_out.reshape(nx, token_rows, width), "x", 0, 0, tiled=True
    )
    results = in_order(outputs(mine), outputs(other), 0)
    returned = lax.all_to_all(
        results.reshape(groups, slot_cap, width), ("x", "y"), 0, 0, tiled=True
    ).reshape(slots, width)
    source_out = jnp.sum(line_back.astype(jnp.float32), axis=0).astype(jnp.bfloat16)
    mixed = jnp.dot(blend, returned.astype(jnp.float32), precision=lax.Precision.HIGHEST)
    mixed = mixed + source_mix[:, None] * source_out.astype(jnp.float32)
    return mixed.astype(jnp.bfloat16)


def solution(mesh):
    split = Mesh(
        mesh.devices.reshape(CHIPS_Z, CORES, CHIPS_X, CHIPS_Y), ("z", "c", "x", "y")
    )
    ep, dp = ("z", "c"), ("x", "y")
    return jax.shard_map(
        per_device,
        mesh=split,
        in_specs=(
            P(dp, ep),
            P(dp, ep, None),
            P(dp, ep, None),
            P(dp, None, ep),
            P(dp, None),
            P(dp, None),
            P(),
        ),
        out_specs=P(dp, ep),
        check_vma=False,
    )
```

```python
import jax
import jax.numpy as jnp
from jax import lax
from jax.sharding import Mesh
from jax.sharding import PartitionSpec as P

CHIPS_Z, CORES, CHIPS_X, CHIPS_Y = 8, 2, 8, 8


def from_source(blocks, axis, count, source):
    distance = (lax.axis_index(axis) - source + count) % count
    classes = min(4, count)

    def branch(first):
        def run(sent):
            kept = sent[0]
            for k in range(1, count):
                apart = 2 if k in (1, count - 1) else classes
                pairs = [(root, (root + k) % count) for root in range(first % apart, count, apart)]
                kept = jnp.where(distance == k, lax.ppermute(sent[k], axis, pairs), kept)
            return kept

        return run

    return lax.switch(source % classes, [branch(i) for i in range(classes)], blocks)


def relay_from(block, axis, count, source, chains=1):
    distance = (lax.axis_index(axis) - source + count) % count
    ahead = [(i, (i + 1) % count) for i in range(count)]
    back = [(i, (i - 1) % count) for i in range(count)]
    held = jnp.split(block, chains)
    for step in range(1, count // 2 + 1):
        for part in range(chains):
            sent = held[part]
            kept = jnp.where(distance == step, lax.ppermute(sent, axis, ahead), sent)
            if step < count - step:
                got = lax.ppermute(sent, axis, back)
                kept = jnp.where(distance == count - step, got, kept)
            held[part] = kept
    return jnp.concatenate(held)


def dot(left, right):
    return jnp.dot(left, right, preferred_element_type=jnp.float32)


def per_device(tokens, gate_weight, up_weight, down_weight, targets, mixing, move_plan):
    nz, nc, nx, ny = (lax.axis_size(a) for a in ("z", "c", "x", "y"))
    groups, parts = nx * ny, nz * nc
    core = lax.axis_index("c")
    token_rows, per_token = targets.shape
    width = tokens.shape[1]
    hidden_units = gate_weight.shape[2]
    slot_cap = min(token_rows, max(2, (2 * token_rows * per_token + groups - 1) // groups))
    slots = groups * slot_cap
    half, share = slots // nc, slots // parts
    block_units = hidden_units // nx
    lanes = jnp.arange(groups, dtype=jnp.int32)
    source = jnp.max(jnp.where(move_plan != lanes, move_plan, -1))
    gate, up, down = gate_weight[0], up_weight[0], down_weight[0]

    named = (targets[:, :, None] == lanes).astype(jnp.float32)
    moved = ((move_plan == source) | (lanes == source)).astype(jnp.float32)
    served = jnp.sum(named * moved, axis=2)
    hits = jnp.sum(named * (1.0 - moved), axis=1)
    rank = jnp.arange(token_rows, dtype=jnp.int32)
    before = (rank[None, :] < rank[:, None]).astype(jnp.bfloat16)
    earlier = dot(before, hits.astype(jnp.bfloat16))
    position = jnp.sum(named * earlier[:, None, :], axis=2).astype(jnp.int32)
    destination = jnp.where(served > 0, -1, targets * slot_cap + position)
    places = jnp.arange(slots, dtype=jnp.int32)
    matches = (destination[:, :, None] == places).astype(jnp.float32)
    pick = jnp.sum(matches, axis=1).astype(jnp.bfloat16)
    blend = jnp.sum(matches * mixing[:, :, None], axis=1)
    source_mix = jnp.sum(mixing * served, axis=1)

    outgoing = lax.dot_general(
        pick, tokens, (((0,), (0,)), ((), ())), preferred_element_type=jnp.float32
    ).astype(jnp.bfloat16)
    line_tokens = lax.all_to_all(
        jnp.broadcast_to(tokens, (nx,) + tokens.shape), "x", 0, 0, tiled=True
    ).reshape(nx * token_rows, width)
    outgoing, line_tokens = lax.optimization_barrier((outgoing, line_tokens))
    arrived = lax.all_to_all(
        outgoing.reshape(groups, slot_cap, width), ("x", "y"), 0, 0, tiled=True
    ).reshape(slots, width)

    tall = jnp.concatenate([gate, up, down.T], axis=0)
    pieces = [tall[:, k * block_units : (k + 1) * block_units] for k in range(nx)]
    piece = from_source(pieces, "x", nx, source // ny)
    arrived, piece = lax.optimization_barrier((arrived, piece))

    swap = [(0, 1), (1, 0)]

    def project(side):
        rows = lax.dynamic_slice_in_dim(arrived, side * half, half, 0)
        return jnp.concatenate([dot(rows, gate), dot(rows, up)], axis=1)

    sent = lax.ppermute(project(1 - core).astype(jnp.bfloat16), "c", swap)
    chip_sum = (project(core) + sent.astype(jnp.float32)).astype(jnp.bfloat16)
    spread = lax.all_to_all(
        chip_sum.reshape(nz, share, 2 * hidden_units), "z", 0, 0, tiled=True
    )
    piece = relay_from(piece, "y", ny, source % ny)
    spread, piece = lax.optimization_barrier((spread, piece))
    gate_block, up_block, down_block = piece[:width], piece[width : 2 * width], piece[2 * width :]

    line_share = nx * token_rows // parts
    line_sums = jnp.concatenate(
        [dot(line_tokens, gate_block), dot(line_tokens, up_block)], axis=1
    ).astype(jnp.bfloat16)
    line_parts = lax.all_to_all(
        line_sums.reshape(parts, line_share, 2 * block_units), ("z", "c"), 0, 0, tiled=True
    )
    main = jnp.sum(spread.astype(jnp.float32), axis=0)
    hidden = (jax.nn.silu(main[:, :hidden_units]) * main[:, hidden_units:]).astype(jnp.bfloat16)
    line = jnp.sum(line_parts.astype(jnp.float32), axis=0)
    line_hidden = (jax.nn.silu(line[:, :block_units]) * line[:, block_units:]).astype(jnp.bfloat16)

    def lanes_for(value, count):
        missing = count - value.shape[0]
        return jnp.pad(value, ((0, missing), (0, 0))) if missing else value

    rows_sent = max(share, line_share)
    payload = jnp.concatenate(
        [lanes_for(hidden, rows_sent), lanes_for(line_hidden, rows_sent)], axis=1
    )
    mine = lax.all_to_all(
        jnp.broadcast_to(payload, (nz,) + payload.shape), "z", 0, 0, tiled=True
    )
    other = lax.ppermute(mine, "c", swap)

    def line_outputs(both):
        rows = both[:, :line_share, hidden_units:].reshape(nz * line_share, block_units)
        out = lax.dot_general(
            rows, down_block, (((1,), (1,)), ((), ())), preferred_element_type=jnp.float32
        )
        return out.astype(jnp.bfloat16).reshape(nz, line_share, width)

    def outputs(both):
        rows = both[:, :share, :hidden_units].reshape(half, hidden_units)
        return dot(rows, down).astype(jnp.bfloat16)

    def in_order(a, b, axis):
        first, second = jnp.where(core == 0, a, b), jnp.where(core == 0, b, a)
        return jnp.concatenate([first, second], axis=axis)

    line_out = in_order(line_outputs(mine), line_outputs(other), 1)
    line_back = lax.all_to_all(
        line_out.reshape(nx, token_rows, width), "x", 0, 0, tiled=True
    )
    results = in_order(outputs(mine), outputs(other), 0)
    returned = lax.all_to_all(
        results.reshape(groups, slot_cap, width), ("x", "y"), 0, 0, tiled=True
    ).reshape(slots, width)
    source_out = jnp.sum(line_back.astype(jnp.float32), axis=0).astype(jnp.bfloat16)
    mixed = jnp.dot(blend, returned.astype(jnp.float32), precision=lax.Precision.HIGHEST)
    mixed = mixed + source_mix[:, None] * source_out.astype(jnp.float32)
    return mixed.astype(jnp.bfloat16)


def solution(mesh):
    split = Mesh(
        mesh.devices.reshape(CHIPS_Z, CORES, CHIPS_X, CHIPS_Y), ("z", "c", "x", "y")
    )
    ep, dp = ("z", "c"), ("x", "y")
    return jax.shard_map(
        per_device,
        mesh=split,
        in_specs=(
            P(dp, ep),
            P(dp, ep, None),
            P(dp, ep, None),
            P(dp, None, ep),
            P(dp, None),
            P(dp, None),
            P(),
        ),
        out_specs=P(dp, ep),
        check_vma=False,
    )
```
